512 devices in a mesh: gx: 32 (over z, core), gy: 16 (over x, y).
Axes of the slice: x: 4, y: 4, z: 16, core: 2. Of those that a mesh axis runs over, the one named last changes fastest.
Arguments:
- blocks: bfloat16 [32, 16, 3, 320, 2240], P('gx', 'gy'), may hold values from -1 to 2
- right_side: bfloat16 [32, 16, 3, 320, 128], P('gx', 'gy'), may hold values from -6 to 6
- departure: int32 [32, 16, 2], P('gx', 'gy'), may hold values from -1 to 2, as said below
- arrival: int32 [32, 16, 2], P('gx', 'gy'), may hold values from 0 to 4, as said below
- neighbors: int32 [32, 16, 2, 6], P('gx', 'gy'), may hold values from 0 to 5, as said below
- orientation: int32 [32, 16, 2, 6], P('gx', 'gy'), may hold values from 0 to 3
Outputs:
- smoothed: float32 [32, 16, 2, 320, 128], P('gx', 'gy')
The draws below stay inside these ranges and needn't reach their ends.
Inputs may be any that keep to these rules, and one draw needn't show every extreme that they name: Position (l, c) holds its rows in some of its 3 slots; its live slots are exactly those named in its departure or arrival entries, each once. At most one of the two entries is a slot; the device with c = 0 never sends lower, the one with c = 15 never upper. Every position holds 1 to 3 rows before and exactly 2 after; in every layer some position holds 3. `arrival`: values below 3 name a local slot, kept in rising order; 3 is the row that the lower gy neighbour sends upward, 4 the one the upper neighbour sends downward, consistent with departure. `neighbors`: face 0 names 0 or 1, face 1 names 4 or 5; no entry of row q names 2 + q.
All inputs are finite; a program needn't handle non-finite values.
Results may differ from the reference program's by a relative error of at most 0.0035.
Values may be sent and summed in bfloat16 or wider, within the bound.
No kernel may reach another device: no remote copies, remote signals or barrier semaphores. Data moves between devices by JAX's collectives and lax.ppermute only.
A program may use at most 64 MiB of HBM per device.

```python
import math
import jax
import jax.numpy as jnp
from jax import lax

VARS = 5
NODES = 4
DOF = 320
FACES = 6
SLOTS = 3
KEPT = 2
RHS = 128
ITERS = 4
LAYERS = 32
COLUMNS = 16


def balance_plan(key):
    sign_key, moving_key, forced_key, slot_key = jax.random.split(jax.random.fold_in(key, 7), 4)
    edge_shape = (LAYERS, COLUMNS - 1)
    signs = 2 * jax.random.randint(sign_key, edge_shape, 0, 2) - 1
    moving = jax.random.randint(moving_key, edge_shape, 0, 2)
    forced = jax.random.randint(forced_key, (LAYERS, 1), 0, COLUMNS - 1)
    edges = jnp.arange(COLUMNS - 1, dtype=jnp.int32)[None, :]
    signs = jnp.where(edges == forced, 1, signs)
    moving = jnp.where(edges == forced, 1, jnp.where(edges == forced - 1, 0, moving))
    flows = signs * moving
    earlier = jnp.pad(flows[:, :-1], ((0, 0), (1, 0)))
    flows = jnp.where(earlier * flows < 0, 0, flows)
    upper_edge = jnp.pad(flows, ((0, 0), (0, 1)))
    lower_edge = jnp.pad(flows, ((0, 0), (1, 0)))
    out_upper = (upper_edge == 1).astype(jnp.int32)
    out_lower = (lower_edge == -1).astype(jnp.int32)
    in_lower = (lower_edge == 1).astype(jnp.int32)
    in_upper = (upper_edge == -1).astype(jnp.int32)
    live_count = 2 + out_upper + out_lower - in_lower - in_upper
    leaving = jax.random.randint(slot_key, (LAYERS, COLUMNS), 0, live_count)
    departs = out_lower + out_upper
    departure = jnp.stack([jnp.where(out_lower > 0, leaving, -1), jnp.where(out_upper > 0, leaving, -1)], axis=-1)
    kept_count = live_count - departs
    slot_ids = jnp.arange(KEPT, dtype=jnp.int32)[None, None, :]
    local = jnp.where((departs[..., None] > 0) & (slot_ids >= leaving[..., None]), slot_ids + 1, slot_ids)
    incoming = jnp.where(in_lower > 0, SLOTS, SLOTS + 1)[..., None]
    arrival = jnp.where(slot_ids < kept_count[..., None], local, incoming)
    return (departure.astype(jnp.int32), arrival.astype(jnp.int32))


def draw_departure(key, part):
    return balance_plan(key)[0]


def draw_arrival(key, part):
    return balance_plan(key)[1]


def draw_neighbors(key, part):
    lower_key, upper_key, other_key = jax.random.split(jax.random.fold_in(key, 11), 3)
    lower = jax.random.randint(lower_key, (LAYERS, COLUMNS, KEPT, 1), 0, 2)
    upper = 4 + jax.random.randint(upper_key, (LAYERS, COLUMNS, KEPT, 1), 0, 2)
    others = jax.random.randint(other_key, (LAYERS, COLUMNS, KEPT, FACES - 2), 0, 5)
    itself = 2 + jnp.arange(KEPT, dtype=jnp.int32)[None, None, :, None]
    others = others + (others >= itself).astype(jnp.int32)
    return jnp.concatenate([lower, upper, others], axis=-1).astype(jnp.int32)


def draw_blocks(key, part):
    shape = (LAYERS, COLUMNS, SLOTS, DOF, 7 * DOF)
    noise_key = jax.random.fold_in(jax.random.fold_in(key, 3), 0)
    column_ids = jnp.arange(7 * DOF)[None, :]
    row_ids = jnp.arange(DOF)[:, None]
    spread = jnp.where(column_ids < DOF, 0.3, 0.15) / math.sqrt(DOF)
    noise = jax.random.normal(noise_key, shape, jnp.float32)
    identity = (column_ids == row_ids).astype(jnp.float32)
    return (identity + spread * noise).astype(jnp.bfloat16)


def set_ends(entries, key, least, high):
    dims = entries.shape
    spot = [jax.random.randint(jax.random.fold_in(key, axis), (), 0, dims[axis]) for axis in range(len(dims))]
    entries = entries.at[tuple(spot)].set(least)
    longest = dims.index(max(dims))
    spot[longest] = (spot[longest] + 1) % dims[longest]
    return entries.at[tuple(spot)].set(high)


def block_levels(rng, shape, cuts, least, high):
    level, own = 1.0, jax.random.fold_in(rng, 6)
    for axis_at, blocks in cuts:
        draws = jnp.exp(jax.random.uniform(jax.random.fold_in(own, axis_at), (blocks,), jnp.float32, least / len(cuts), high / len(cuts)))
        level = level * jnp.repeat(draws, shape[axis_at] // blocks).reshape([-1 if axis == axis_at else 1 for axis in range(len(shape))])
    return level


def normal_values(stream_key, shape, deviation, most, cuts=(), kind=jnp.bfloat16):
    values = deviation * jax.random.normal(stream_key, shape, jnp.float32)
    if cuts:
        values = values * block_levels(stream_key, shape, cuts, -0.22, 0.18)
    return jnp.clip(values, -most, most).astype(kind)


def setup_inputs(seed: int = 0) -> dict:
    arg_keys = jax.random.split(jax.random.key(seed), 7)
    blocks = draw_blocks(jax.random.fold_in(arg_keys[6], 71), 0)
    right_side = normal_values(arg_keys[1], (LAYERS, COLUMNS, SLOTS, DOF, RHS), 1.0, 6.0, ((0, 32), (1, 16)))
    departure = draw_departure(jax.random.fold_in(arg_keys[6], 71), 0)
    arrival = draw_arrival(jax.random.fold_in(arg_keys[6], 71), 0)
    neighbors = draw_neighbors(jax.random.fold_in(arg_keys[6], 71), 0)
    orientation = set_ends(jax.random.randint(arg_keys[5], (LAYERS, COLUMNS, KEPT, FACES), 0, 4), jax.random.fold_in(arg_keys[5], 1), 0, 3).astype(jnp.int32)
    return dict(blocks=blocks, right_side=right_side, departure=departure, arrival=arrival, neighbors=neighbors, orientation=orientation)


RELAXATION = 0.7


def turned_faces(faces, face_codes):
    nodal = faces.reshape(faces.shape[:-2] + (VARS, NODES, NODES, NODES, faces.shape[-1]))
    result = nodal
    for quarter in range(1, 4):
        picked = (face_codes == quarter).reshape(face_codes.shape + (1, 1, 1, 1, 1))
        result = jnp.where(picked, jnp.rot90(nodal, quarter, axes=(-4, -3)), result)
    return result.reshape(faces.shape)


def reference(blocks, right_side, departure, arrival, neighbors, orientation):
    layers = arrival.shape[0]
    columns = arrival.shape[1]
    column_ids = jnp.arange(columns, dtype=jnp.int32)
    from_lower_slot = jnp.roll(departure[:, :, 1], 1, axis=1)[:, :, None]
    from_upper_slot = jnp.roll(departure[:, :, 0], -1, axis=1)[:, :, None]
    source_column = column_ids[None, :, None] + (arrival == SLOTS + 1).astype(jnp.int32) - (arrival == SLOTS).astype(jnp.int32)
    source_slot = jnp.where(arrival < SLOTS, arrival, jnp.where(arrival == SLOTS, from_lower_slot, from_upper_slot))
    layer_ids = jnp.arange(layers, dtype=jnp.int32)[:, None, None]
    row_rhs = right_side[layer_ids, source_column, source_slot].astype(jnp.float32)
    iterate = RELAXATION * row_rhs
    for sweep_index in range(ITERS):
        rounded = iterate.astype(jnp.bfloat16)
        padded = jnp.pad(rounded, ((1, 1), (0, 0), (0, 0), (0, 0), (0, 0)))

        def layer_image(layer_number):
            window = lax.dynamic_slice_in_dim(padded, layer_number, 3, 0)
            window = jnp.moveaxis(window, 1, 0).reshape(columns, 3 * KEPT, DOF, RHS)
            layer_rows = blocks[layer_number][source_column[layer_number], source_slot[layer_number]]
            faces = window[column_ids[:, None, None], neighbors[layer_number]]
            faces = turned_faces(faces, orientation[layer_number])
            stacked = jnp.concatenate([rounded[layer_number][:, :, None], faces], axis=2)
            stacked = stacked.reshape(columns, KEPT, 7 * DOF, RHS).astype(jnp.float32)
            return jnp.einsum("cqde,cqer->cqdr", layer_rows.astype(jnp.float32), stacked, precision=lax.Precision.HIGHEST)

        applied = lax.map(layer_image, jnp.arange(layers, dtype=jnp.int32))
        iterate = iterate + RELAXATION * (row_rhs - applied)
    return iterate
```

```python
import jax
import jax.numpy as jnp
from jax import lax
from jax.experimental import pallas as pl
from jax.experimental.pallas import tpu as pltpu
from jax.sharding import PartitionSpec as P

DOF = 320
FACES = 6
RHS = 128
KEPT = 2
ITERS = 4
RELAXATION = 0.7
WIDE = 7 * DOF
TILE = 128
SLOTS = 6
MERGED = SLOTS * DOF
TILES = MERGED // TILE
HEAD = 2
META = 16


def vmem(shape, dtype):
    return pltpu.VMEM(shape, dtype)


def near(*arrays):
    return tuple(pltpu.with_memory_space_constraint(array, pltpu.VMEM) for array in arrays)


def far(*arrays):
    return tuple(pltpu.with_memory_space_constraint(array, pltpu.HBM) for array in arrays)


PARAMS = pltpu.CompilerParams(vmem_limit_bytes=20 * 2**20)

SMEM_SPEC = pl.BlockSpec(memory_space=pltpu.SMEM)
VMEM_SPEC = pl.BlockSpec(memory_space=pltpu.VMEM)
ANY_SPEC = pl.BlockSpec(memory_space=pl.ANY)


def merge_row(row_ref, neighbor, turn, row, parity, acc_ref):
    lane = lax.broadcasted_iota(jnp.int32, (DOF, TILE), 1)
    for tile in range(HEAD):
        acc_ref[tile] = row_ref[:, tile * TILE : (tile + 1) * TILE].astype(jnp.float32)
    edge = row_ref[:, HEAD * TILE : (HEAD + 1) * TILE].astype(jnp.float32)
    acc_ref[HEAD] = jnp.where(lane < DOF - HEAD * TILE, edge, 0.0)
    for tile in range(HEAD + 1, TILES):
        acc_ref[tile] = jnp.zeros((DOF, TILE), jnp.float32)
    for face in range(FACES):
        start = DOF * (face + 1)
        shift = start % TILE
        base = start - shift
        width = DOF + shift
        n = neighbor(face)
        k = turn(face)
        layer = n // 2
        which = n % 2
        first = jnp.where(parity == 0, layer == 2, layer == 0)
        slot = jnp.where(layer == 1, 1, jnp.where(first, 2, 4) + which)
        place = DOF * slot
        tile = place // TILE
        offset = place - tile * TILE
        column = lax.broadcasted_iota(jnp.int32, (1, 3 * TILE), 1) - offset
        a = (column // 16) % 4
        b = (column // 4) % 4
        source_a = jnp.where(k == 0, a, jnp.where(k == 1, 3 - b, jnp.where(k == 2, 3 - a, b)))
        source_b = jnp.where(k == 0, b, jnp.where(k == 1, a, jnp.where(k == 2, 3 - b, 3 - a)))
        source = shift + (column // 64) * 64 + source_a * 16 + source_b * 4 + column % 4
        source = jnp.where((column >= 0) & (column < DOF), source, -1)
        rows = lax.broadcasted_iota(jnp.int32, (width, 3 * TILE), 0)
        select = jnp.where(rows == source, 1.0, 0.0).astype(jnp.bfloat16)
        moved = jnp.dot(row_ref[:, base : base + width], select, preferred_element_type=jnp.float32)
        for part in range(3):
            acc_ref[tile + part] += moved[:, part * TILE : (part + 1) * TILE]


def pick_kernel(departure, arrival, neighbors, orientation, blocks, rhs, head, row, meta_down, meta_up, sems):
    slot = jnp.maximum(jnp.maximum(departure[0, 0, 0], departure[0, 0, 1]), 0)
    whole = pltpu.make_async_copy(blocks.at[0, 0, slot], row, sems.at[0])
    side = pltpu.make_async_copy(rhs.at[0, 0, slot], head.at[:, 0:RHS], sems.at[1])
    whole.start()
    side.start()
    for meta, code in ((meta_down, 3), (meta_up, 4)):
        q = jnp.where(arrival[0, 0, 1] == code, 1, 0)
        for face in range(FACES):
            meta[face] = neighbors[0, 0, q, face]
            meta[FACES + face] = orientation[0, 0, q, face]
        for index in range(2 * FACES, META):
            meta[index] = q
    whole.wait()
    side.wait()
    head[:, RHS:] = row[:, 0 : HEAD * TILE]


def pick(departure, arrival, neighbors, orientation, blocks, rhs):
    return pl.pallas_call(
        pick_kernel,
        in_specs=[SMEM_SPEC] * 4 + [ANY_SPEC] * 2,
        out_specs=[VMEM_SPEC, VMEM_SPEC, SMEM_SPEC, SMEM_SPEC],
        out_shape=[
            vmem((DOF, RHS + HEAD * TILE), jnp.bfloat16),
            vmem((DOF, WIDE), jnp.bfloat16),
            jax.ShapeDtypeStruct((META,), jnp.int32),
            jax.ShapeDtypeStruct((META,), jnp.int32),
        ],
        scratch_shapes=[pltpu.SemaphoreType.DMA((2,))],
        compiler_params=PARAMS,
        name="pick",
    )(*far(departure, arrival, neighbors, orientation, blocks, rhs))


def send_kernel(departure, from_upper, from_lower, row, tail, acc):
    parity = lax.axis_index("gx") % 2
    up = departure[0, 0, 1] >= 0

    def entry(index):
        return jnp.where(up, from_upper[index], from_lower[index])

    merge_row(row, entry, lambda face: entry(FACES + face), entry(2 * FACES), parity, acc)
    for tile in range(HEAD, TILES):
        tail[:, (tile - HEAD) * TILE : (tile - HEAD + 1) * TILE] = acc[tile].astype(jnp.bfloat16)


def merged_tail(departure, from_upper, from_lower, row):
    return pl.pallas_call(
        send_kernel,
        in_specs=[SMEM_SPEC] * 3 + [VMEM_SPEC],
        out_specs=VMEM_SPEC,
        out_shape=vmem((DOF, (TILES - HEAD) * TILE), jnp.bfloat16),
        scratch_shapes=[pltpu.VMEM((TILES, DOF, TILE), jnp.float32)],
        compiler_params=PARAMS,
        name="merge_tail",
    )(departure, from_upper, from_lower, *near(row))


def first_kernel(arrival, rhs, lower, upper, kept, rounded):
    for q in range(KEPT):
        source = arrival[0, 0, q]

        @pl.when(source < 3)
        def _():
            kept[q] = rhs[0, 0, jnp.clip(source, 0, 2)]

        @pl.when(source == 3)
        def _():
            kept[q] = lower[:, 0:RHS]

        @pl.when(source == 4)
        def _():
            kept[q] = upper[:, 0:RHS]

        rounded[q] = (RELAXATION * kept[q].astype(jnp.float32)).astype(jnp.bfloat16)


def first(arrival, rhs, lower, upper):
    pair = vmem((KEPT, DOF, RHS), jnp.bfloat16)
    return pl.pallas_call(
        first_kernel,
        in_specs=[SMEM_SPEC] + [VMEM_SPEC] * 3,
        out_specs=[VMEM_SPEC] * 2,
        out_shape=[pair, pair],
        compiler_params=PARAMS,
        name="first",
    )(arrival, *near(rhs, lower, upper))


def local_kernel(arrival, neighbors, orientation, blocks, merged, rows, acc, sems):
    parity = lax.axis_index("gx") % 2
    copies = [
        pltpu.make_async_copy(blocks.at[0, 0, jnp.clip(arrival[0, 0, q], 0, 2)], rows.at[q], sems.at[q])
        for q in range(KEPT)
    ]
    for copy in copies:
        copy.start()
    for q in range(KEPT):
        copies[q].wait()
        merge_row(
            rows.at[q], lambda face: neighbors[0, 0, q, face], lambda face: orientation[0, 0, q, face], q, parity, acc
        )
        for tile in range(TILES):
            merged[q, :, tile * TILE : (tile + 1) * TILE] = acc[tile].astype(jnp.bfloat16)


def merged_local(arrival, neighbors, orientation, blocks):
    return pl.pallas_call(
        local_kernel,
        in_specs=[SMEM_SPEC] * 3 + [ANY_SPEC],
        out_specs=VMEM_SPEC,
        out_shape=vmem((KEPT, DOF, MERGED), jnp.bfloat16),
        scratch_shapes=[
            pltpu.VMEM((KEPT, DOF, WIDE), jnp.bfloat16),
            pltpu.VMEM((TILES, DOF, TILE), jnp.float32),
            pltpu.SemaphoreType.DMA((KEPT,)),
        ],
        compiler_params=PARAMS,
        name="merge_local",
    )(arrival, neighbors, orientation, *far(blocks))


def applied_rows(merged, own, pair_a, pair_b):
    far = jnp.concatenate([pair_a[0], pair_a[1], pair_b[0], pair_b[1]], axis=0)
    for q in range(KEPT):
        near = jnp.concatenate([own[q], own[1 - q]], axis=0)
        applied = jnp.dot(merged[q, :, 0 : 2 * DOF], near, preferred_element_type=jnp.float32)
        applied += jnp.dot(merged[q, :, 2 * DOF :], far, preferred_element_type=jnp.float32)
        yield q, applied


def opening_kernel(arrival, local, lo_head, lo_tail, hi_head, hi_tail, kept, own, pair_a, pair_b, merged, iterate, rounded):
    for q in range(KEPT):
        source = arrival[0, 0, q]
        for code, head, tail in ((3, lo_head, lo_tail), (4, hi_head, hi_tail)):

            @pl.when(source == code)
            def _():
                merged[q, :, 0 : HEAD * TILE] = head[:, RHS:]
                merged[q, :, HEAD * TILE :] = tail[...]

        @pl.when(source < 3)
        def _():
            merged[q] = local[q]

    for q, applied in applied_rows(merged, own, pair_a, pair_b):
        side = kept[q].astype(jnp.float32)
        value = RELAXATION * side + RELAXATION * (side - applied)
        iterate[q] = value
        rounded[q] = value.astype(jnp.bfloat16)


def opening(arrival, local, lo_head, lo_tail, hi_head, hi_tail, kept, own, pair_a, pair_b):
    return pl.pallas_call(
        opening_kernel,
        in_specs=[SMEM_SPEC] + [VMEM_SPEC] * 9,
        out_specs=[VMEM_SPEC] * 3,
        out_shape=[
            vmem((KEPT, DOF, MERGED), jnp.bfloat16),
            vmem((KEPT, DOF, RHS), jnp.float32),
            vmem((KEPT, DOF, RHS), jnp.bfloat16),
        ],
        compiler_params=PARAMS,
        name="opening",
    )(arrival, *near(local, lo_head, lo_tail, hi_head, hi_tail, kept, own, pair_a, pair_b))


def middle_kernel(merged, kept, iterate, own, pair_a, pair_b, iterate_out, rounded):
    for q, applied in applied_rows(merged, own, pair_a, pair_b):
        value = iterate[q] + RELAXATION * (kept[q].astype(jnp.float32) - applied)
        iterate_out[q] = value
        rounded[q] = value.astype(jnp.bfloat16)


def middle(merged, kept, iterate, own, pair_a, pair_b):
    return pl.pallas_call(
        middle_kernel,
        in_specs=[VMEM_SPEC] * 6,
        out_specs=[VMEM_SPEC] * 2,
        out_shape=[vmem((KEPT, DOF, RHS), jnp.float32), vmem((KEPT, DOF, RHS), jnp.bfloat16)],
        compiler_params=PARAMS,
        name="middle",
    )(*near(merged, kept, iterate, own, pair_a, pair_b))


def closing_kernel(merged, kept, iterate, own, pair_a, pair_b, smoothed):
    for q, applied in applied_rows(merged, own, pair_a, pair_b):
        smoothed[0, 0, q] = iterate[q] + RELAXATION * (kept[q].astype(jnp.float32) - applied)


def closing(merged, kept, iterate, own, pair_a, pair_b):
    return pl.pallas_call(
        closing_kernel,
        in_specs=[VMEM_SPEC] * 6,
        out_specs=VMEM_SPEC,
        out_shape=jax.ShapeDtypeStruct((1, 1, KEPT, DOF, RHS), jnp.float32),
        compiler_params=PARAMS,
        name="closing",
    )(*near(merged, kept, iterate, own, pair_a, pair_b))


def shifted(value, axis, steps):
    count = lax.axis_size(axis)
    leading, last = (max(0, -steps), min(count, count - steps))
    return lax.ppermute(value, axis, [(source, source + steps) for source in range(leading, last)])


def swapped(value, axis, start):
    count = lax.axis_size(axis)
    pairs = []
    for low in range(start, count - 1, 2):
        pairs += [(low, low + 1), (low + 1, low)]
    return lax.ppermute(value, axis, pairs)


def halo(rounded):
    pair_b = swapped(rounded, "gx", 1)
    pair_a = swapped(rounded, "gx", 0)
    return pair_a, pair_b


def shards(blocks, right_side, departure, arrival, neighbors, orientation):
    head, row, meta_down, meta_up = pick(departure, arrival, neighbors, orientation, blocks, right_side)
    meta_upper = shifted(meta_down, "gy", -1)
    meta_lower = shifted(meta_up, "gy", 1)
    lo_head = shifted(head, "gy", 1)
    hi_head = shifted(head, "gy", -1)
    tail = merged_tail(departure, meta_upper, meta_lower, row)
    lo_tail = shifted(tail, "gy", 1)
    hi_tail = shifted(tail, "gy", -1)
    kept, own = first(arrival, right_side, lo_head, hi_head)
    pair_a, pair_b = halo(own)
    local = merged_local(arrival, neighbors, orientation, blocks)
    merged, iterate, own = opening(
        arrival, local, lo_head, lo_tail, hi_head, hi_tail, kept, own, pair_a, pair_b
    )
    for _ in range(ITERS - 2):
        pair_a, pair_b = halo(own)
        iterate, own = middle(merged, kept, iterate, own, pair_a, pair_b)
    pair_a, pair_b = halo(own)
    return closing(merged, kept, iterate, own, pair_a, pair_b)


def solution(mesh):
    in_specs = (
        P("gx", "gy", None, None, None),
        P("gx", "gy", None, None, None),
        P("gx", "gy", None),
        P("gx", "gy", None),
        P("gx", "gy", None, None),
        P("gx", "gy", None, None),
    )
    out_specs = P("gx", "gy", None, None, None)
    return jax.shard_map(shards, mesh=mesh, in_specs=in_specs, out_specs=out_specs, check_vma=False)
```

```python
import jax
import jax.numpy as jnp
from jax import lax
from jax.experimental import pallas as pl
from jax.experimental.pallas import tpu as pltpu
from jax.sharding import PartitionSpec as P


DOF = 320
FACES = 6
RHS = 128
KEPT = 2
ITERS = 4
RELAXATION = 0.7
WIDE = 7 * DOF
TILE = 128
SLOTS = 6
MERGED = SLOTS * DOF
TILES = MERGED // TILE
HEAD = 2
SPAN = 3
LAST = DOF * FACES


def vmem(shape, dtype):
    return pltpu.VMEM(shape, dtype)


def near(*arrays):
    return tuple(pltpu.with_memory_space_constraint(array, pltpu.VMEM) for array in arrays)


def far(*arrays):
    return tuple(pltpu.with_memory_space_constraint(array, pltpu.HBM) for array in arrays)


PARAMS = pltpu.CompilerParams(vmem_limit_bytes=20 * 2**20)

SMEM_SPEC = pl.BlockSpec(memory_space=pltpu.SMEM)
VMEM_SPEC = pl.BlockSpec(memory_space=pltpu.VMEM)
ANY_SPEC = pl.BlockSpec(memory_space=pl.ANY)


def turned_select(start, n, k, parity):
    shift = start % TILE
    layer = n // 2
    first = jnp.where(parity == 0, layer == 2, layer == 0)
    slot = jnp.where(layer == 1, 1, jnp.where(first, 2, 4) + n % 2)
    place = DOF * slot
    tile = place // TILE
    column = lax.broadcasted_iota(jnp.int32, (1, SPAN * TILE), 1) - (place - tile * TILE)
    a = (column // 16) % 4
    b = (column // 4) % 4
    source_a = jnp.where(k == 0, a, jnp.where(k == 1, 3 - b, jnp.where(k == 2, 3 - a, b)))
    source_b = jnp.where(k == 0, b, jnp.where(k == 1, a, jnp.where(k == 2, 3 - b, 3 - a)))
    source = shift + (column // 64) * 64 + source_a * 16 + source_b * 4 + column % 4
    source = jnp.where((column >= 0) & (column < DOF), source, -1)
    rows = lax.broadcasted_iota(jnp.int32, (DOF + shift, SPAN * TILE), 0)
    return tile, jnp.where(rows == source, 1.0, 0.0).astype(jnp.bfloat16)


def add_faces(faces, columns, neighbor, turn, parity, acc_ref):
    for face in faces:
        start = DOF * (face + 1)
        tile, select = turned_select(start, neighbor(face), turn(face), parity)
        base = start - start % TILE
        moved = jnp.dot(columns(base, start + DOF), select, preferred_element_type=jnp.float32)
        for part in range(SPAN):
            acc_ref[tile + part] += moved[:, part * TILE : (part + 1) * TILE]


def put_own(columns, acc_ref):
    lane = lax.broadcasted_iota(jnp.int32, (DOF, TILE), 1)
    for tile in range(TILES):
        if tile <= HEAD:
            acc_ref[tile] = columns(tile * TILE, (tile + 1) * TILE).astype(jnp.float32)
        else:
            acc_ref[tile] = jnp.zeros((DOF, TILE), jnp.float32)
    acc_ref[HEAD] = jnp.where(lane < DOF - HEAD * TILE, acc_ref[HEAD], 0.0)


def pick_kernel(departure, blocks, rhs, head, middle, last, row, sems):
    slot = jnp.maximum(jnp.maximum(departure[0, 0, 0], departure[0, 0, 1]), 0)
    whole = pltpu.make_async_copy(blocks.at[0, 0, slot], row, sems.at[0])
    side = pltpu.make_async_copy(rhs.at[0, 0, slot], head.at[:, 0:RHS], sems.at[1])
    whole.start()
    side.start()
    whole.wait()
    side.wait()
    head[:, RHS:] = row[:, 0 : HEAD * TILE]
    middle[...] = row[:, HEAD * TILE : LAST]
    last[...] = row[:, LAST:]


def pick(departure, blocks, rhs):
    return pl.pallas_call(
        pick_kernel,
        in_specs=[SMEM_SPEC] + [ANY_SPEC] * 2,
        out_specs=[VMEM_SPEC] * 3,
        out_shape=[
            vmem((DOF, RHS + HEAD * TILE), jnp.bfloat16),
            vmem((DOF, LAST - HEAD * TILE), jnp.bfloat16),
            vmem((DOF, DOF), jnp.bfloat16),
        ],
        scratch_shapes=[pltpu.VMEM((DOF, WIDE), jnp.bfloat16), pltpu.SemaphoreType.DMA((2,))],
        compiler_params=PARAMS,
        name="pick",
    )(*far(departure, blocks, rhs))


def first_kernel(arrival, rhs, lower, upper, kept, rounded):
    for q in range(KEPT):
        source = arrival[0, 0, q]

        @pl.when(source < 3)
        def _():
            kept[q] = rhs[0, 0, jnp.clip(source, 0, 2)]

        @pl.when(source == 3)
        def _():
            kept[q] = lower[:, 0:RHS]

        @pl.when(source == 4)
        def _():
            kept[q] = upper[:, 0:RHS]

        rounded[q] = (RELAXATION * kept[q].astype(jnp.float32)).astype(jnp.bfloat16)


def first(arrival, rhs, lower, upper):
    pair = vmem((KEPT, DOF, RHS), jnp.bfloat16)
    return pl.pallas_call(
        first_kernel,
        in_specs=[SMEM_SPEC] + [VMEM_SPEC] * 3,
        out_specs=[VMEM_SPEC] * 2,
        out_shape=[pair, pair],
        compiler_params=PARAMS,
        name="first",
    )(arrival, *near(rhs, lower, upper))


def local_kernel(arrival, neighbors, orientation, blocks, merged, rows, acc, sems):
    parity = lax.axis_index("gx") % 2
    copies = [
        pltpu.make_async_copy(blocks.at[0, 0, jnp.clip(arrival[0, 0, q], 0, 2)], rows.at[q], sems.at[q])
        for q in range(KEPT)
    ]
    for copy in copies:
        copy.start()
    for q in range(KEPT):
        copies[q].wait()

        @pl.when(arrival[0, 0, q] < 3)
        def _():
            columns = lambda low, high: rows[q, :, low:high]
            put_own(columns, acc)
            neighbor = lambda face: neighbors[0, 0, q, face]
            turn = lambda face: orientation[0, 0, q, face]
            add_faces(range(FACES), columns, neighbor, turn, parity, acc)
            for tile in range(TILES):
                merged[q, :, tile * TILE : (tile + 1) * TILE] = acc[tile].astype(jnp.bfloat16)


def merged_local(arrival, neighbors, orientation, blocks):
    return pl.pallas_call(
        local_kernel,
        in_specs=[SMEM_SPEC] * 3 + [ANY_SPEC],
        out_specs=VMEM_SPEC,
        out_shape=vmem((KEPT, DOF, MERGED), jnp.bfloat16),
        scratch_shapes=[
            pltpu.VMEM((KEPT, DOF, WIDE), jnp.bfloat16),
            pltpu.VMEM((TILES, DOF, TILE), jnp.float32),
            pltpu.SemaphoreType.DMA((KEPT,)),
        ],
        compiler_params=PARAMS,
        name="merge_local",
    )(arrival, neighbors, orientation, *far(blocks))


def arrived_kernel(
    arrival, neighbors, orientation, local, lo_head, lo_middle, hi_head, hi_middle, merged, acc
):
    del local
    parity = lax.axis_index("gx") % 2
    for q in range(KEPT):
        for code, head, middle in ((3, lo_head, lo_middle), (4, hi_head, hi_middle)):

            @pl.when(arrival[0, 0, q] == code)
            def _():
                def columns(low, high):
                    if high <= HEAD * TILE:
                        return head[:, RHS + low : RHS + high]
                    return middle[:, low - HEAD * TILE : high - HEAD * TILE]

                put_own(columns, acc.at[q])
                neighbor = lambda face: neighbors[0, 0, q, face]
                turn = lambda face: orientation[0, 0, q, face]
                add_faces(range(FACES - 1), columns, neighbor, turn, parity, acc.at[q])
                for tile in range(TILES):
                    merged[q, :, tile * TILE : (tile + 1) * TILE] = acc[q, tile].astype(jnp.bfloat16)


def merged_arrived(arrival, neighbors, orientation, local, lo_head, lo_middle, hi_head, hi_middle):
    return pl.pallas_call(
        arrived_kernel,
        in_specs=[SMEM_SPEC] * 3 + [VMEM_SPEC] * 5,
        out_specs=[VMEM_SPEC] * 2,
        out_shape=[
            vmem((KEPT, DOF, MERGED), jnp.bfloat16),
            vmem((KEPT, TILES, DOF, TILE), jnp.float32),
        ],
        input_output_aliases={3: 0},
        compiler_params=PARAMS,
        name="merge_arrived",
    )(arrival, neighbors, orientation, *near(local, lo_head, lo_middle, hi_head, hi_middle))


def applied_rows(merged, own, pair_a, pair_b):
    far = jnp.concatenate([pair_a[0], pair_a[1], pair_b[0], pair_b[1]], axis=0)
    for q in range(KEPT):
        near = jnp.concatenate([own[q], own[1 - q]], axis=0)
        applied = jnp.dot(merged[q, :, 0 : 2 * DOF], near, preferred_element_type=jnp.float32)
        applied += jnp.dot(merged[q, :, 2 * DOF :], far, preferred_element_type=jnp.float32)
        yield q, applied


def opening_kernel(
    arrival, neighbors, orientation, partial, acc, lo_last, hi_last, kept, own, pair_a, pair_b, merged, iterate, rounded
):
    del partial
    parity = lax.axis_index("gx") % 2
    for q in range(KEPT):
        for code, last in ((3, lo_last), (4, hi_last)):

            @pl.when(arrival[0, 0, q] == code)
            def _():
                face = FACES - 1
                tile, select = turned_select(LAST, neighbors[0, 0, q, face], orientation[0, 0, q, face], parity)
                moved = jnp.dot(last[...], select, preferred_element_type=jnp.float32)
                for part in range(SPAN):
                    total = acc[q, tile + part] + moved[:, part * TILE : (part + 1) * TILE]
                    place = pl.multiple_of((tile + part) * TILE, TILE)
                    merged[q, :, pl.ds(place, TILE)] = total.astype(jnp.bfloat16)

    for q, applied in applied_rows(merged, own, pair_a, pair_b):
        side = kept[q].astype(jnp.float32)
        value = RELAXATION * side + RELAXATION * (side - applied)
        iterate[q] = value
        rounded[q] = value.astype(jnp.bfloat16)


def opening(arrival, neighbors, orientation, partial, acc, lo_last, hi_last, kept, own, pair_a, pair_b):
    return pl.pallas_call(
        opening_kernel,
        in_specs=[SMEM_SPEC] * 3 + [VMEM_SPEC] * 8,
        out_specs=[VMEM_SPEC] * 3,
        out_shape=[
            vmem((KEPT, DOF, MERGED), jnp.bfloat16),
            vmem((KEPT, DOF, RHS), jnp.float32),
            vmem((KEPT, DOF, RHS), jnp.bfloat16),
        ],
        input_output_aliases={3: 0},
        compiler_params=PARAMS,
        name="opening",
    )(arrival, neighbors, orientation, *near(partial, acc, lo_last, hi_last, kept, own, pair_a, pair_b))


def middle_kernel(merged, kept, iterate, own, pair_a, pair_b, iterate_out, rounded):
    for q, applied in applied_rows(merged, own, pair_a, pair_b):
        value = iterate[q] + RELAXATION * (kept[q].astype(jnp.float32) - applied)
        iterate_out[q] = value
        rounded[q] = value.astype(jnp.bfloat16)


def middle(merged, kept, iterate, own, pair_a, pair_b):
    return pl.pallas_call(
        middle_kernel,
        in_specs=[VMEM_SPEC] * 6,
        out_specs=[VMEM_SPEC] * 2,
        out_shape=[vmem((KEPT, DOF, RHS), jnp.float32), vmem((KEPT, DOF, RHS), jnp.bfloat16)],
        compiler_params=PARAMS,
        name="middle",
    )(*near(merged, kept, iterate, own, pair_a, pair_b))


def closing_kernel(merged, kept, iterate, own, pair_a, pair_b, smoothed):
    for q, applied in applied_rows(merged, own, pair_a, pair_b):
        smoothed[0, 0, q] = iterate[q] + RELAXATION * (kept[q].astype(jnp.float32) - applied)


def closing(merged, kept, iterate, own, pair_a, pair_b):
    return pl.pallas_call(
        closing_kernel,
        in_specs=[VMEM_SPEC] * 6,
        out_specs=VMEM_SPEC,
        out_shape=jax.ShapeDtypeStruct((1, 1, KEPT, DOF, RHS), jnp.float32),
        compiler_params=PARAMS,
        name="closing",
    )(*near(merged, kept, iterate, own, pair_a, pair_b))


def shifted(value, axis, steps):
    count = lax.axis_size(axis)
    leading, last = (max(0, -steps), min(count, count - steps))
    return lax.ppermute(value, axis, [(source, source + steps) for source in range(leading, last)])


def swapped(value, axis, start):
    count = lax.axis_size(axis)
    pairs = []
    for low in range(start, count - 1, 2):
        pairs += [(low, low + 1), (low + 1, low)]
    return lax.ppermute(value, axis, pairs)


def halo(rounded):
    pair_b = swapped(rounded, "gx", 1)
    pair_a = swapped(rounded, "gx", 0)
    return pair_a, pair_b


def both_ways(value):
    lower = shifted(value, "gy", 1)
    upper = shifted(value, "gy", -1)
    return lower, upper


def shards(blocks, right_side, departure, arrival, neighbors, orientation):
    head, middle_columns, last = pick(departure, blocks, right_side)
    lo_head, hi_head = both_ways(head)
    lo_middle, hi_middle = both_ways(middle_columns)
    lo_last, hi_last = both_ways(last)
    kept, own = first(arrival, right_side, lo_head, hi_head)
    pair_a, pair_b = halo(own)
    local = merged_local(arrival, neighbors, orientation, blocks)
    partial, acc = merged_arrived(
        arrival, neighbors, orientation, local, lo_head, lo_middle, hi_head, hi_middle
    )
    merged, iterate, own = opening(
        arrival, neighbors, orientation, partial, acc, lo_last, hi_last, kept, own, pair_a, pair_b
    )
    for _ in range(1, ITERS - 1):
        pair_a, pair_b = halo(own)
        iterate, own = middle(merged, kept, iterate, own, pair_a, pair_b)
    pair_a, pair_b = halo(own)
    return closing(merged, kept, iterate, own, pair_a, pair_b)


def solution(mesh):
    in_specs = (
        P("gx", "gy", None, None, None),
        P("gx", "gy", None, None, None),
        P("gx", "gy", None),
        P("gx", "gy", None),
        P("gx", "gy", None, None),
        P("gx", "gy", None, None),
    )
    out_specs = P("gx", "gy", None, None, None)
    return jax.shard_map(shards, mesh=mesh, in_specs=in_specs, out_specs=out_specs, check_vma=False)
```

```python
import jax
import jax.numpy as jnp
from jax import lax
from jax.experimental import pallas as pl
from jax.experimental.pallas import tpu as pltpu
from jax.sharding import PartitionSpec as P


DOF = 320
FACES = 6
RHS = 128
KEPT = 2
ITERS = 4
RELAXATION = 0.7
WIDE = 7 * DOF
TILE = 128
SLOTS = 6
MERGED = SLOTS * DOF
TILES = MERGED // TILE
HEAD = 2
SPAN = 3
LAST = DOF * FACES


def vmem(shape, dtype):
    return pltpu.VMEM(shape, dtype)


def near(*arrays):
    return tuple(pltpu.with_memory_space_constraint(array, pltpu.VMEM) for array in arrays)


def far(*arrays):
    return tuple(pltpu.with_memory_space_constraint(array, pltpu.HBM) for array in arrays)


PARAMS = pltpu.CompilerParams(vmem_limit_bytes=20 * 2**20)

SMEM_SPEC = pl.BlockSpec(memory_space=pltpu.SMEM)
VMEM_SPEC = pl.BlockSpec(memory_space=pltpu.VMEM)
ANY_SPEC = pl.BlockSpec(memory_space=pl.ANY)


def turned_select(start, n, k):
    shift = start % TILE
    layer = n // 2
    here = lax.axis_index("gx")
    outside = ((layer == 0) & (here == 0)) | ((layer == 2) & (here == lax.axis_size("gx") - 1))
    slot = jnp.where(layer == 1, 1, jnp.where(layer == 0, 2, 4) + n % 2)
    place = DOF * slot
    tile = place // TILE
    column = lax.broadcasted_iota(jnp.int32, (1, SPAN * TILE), 1) - (place - tile * TILE)
    a = (column // 16) % 4
    b = (column // 4) % 4
    source_a = jnp.where(k == 0, a, jnp.where(k == 1, 3 - b, jnp.where(k == 2, 3 - a, b)))
    source_b = jnp.where(k == 0, b, jnp.where(k == 1, a, jnp.where(k == 2, 3 - b, 3 - a)))
    source = shift + (column // 64) * 64 + source_a * 16 + source_b * 4 + column % 4
    source = jnp.where((column >= 0) & (column < DOF) & jnp.logical_not(outside), source, -1)
    rows = lax.broadcasted_iota(jnp.int32, (DOF + shift, SPAN * TILE), 0)
    return tile, jnp.where(rows == source, 1.0, 0.0).astype(jnp.bfloat16)


def add_faces(faces, columns, neighbor, turn, acc_ref):
    for face in faces:
        start = DOF * (face + 1)
        tile, select = turned_select(start, neighbor(face), turn(face))
        base = start - start % TILE
        moved = jnp.dot(columns(base, start + DOF), select, preferred_element_type=jnp.float32)
        for part in range(SPAN):
            acc_ref[tile + part] += moved[:, part * TILE : (part + 1) * TILE]


def put_own(columns, acc_ref):
    lane = lax.broadcasted_iota(jnp.int32, (DOF, TILE), 1)
    for tile in range(TILES):
        if tile <= HEAD:
            acc_ref[tile] = columns(tile * TILE, (tile + 1) * TILE).astype(jnp.float32)
        else:
            acc_ref[tile] = jnp.zeros((DOF, TILE), jnp.float32)
    acc_ref[HEAD] = jnp.where(lane < DOF - HEAD * TILE, acc_ref[HEAD], 0.0)


def pick_kernel(departure, blocks, rhs, head, middle, last, row, sems):
    slot = jnp.maximum(jnp.maximum(departure[0, 0, 0], departure[0, 0, 1]), 0)
    whole = pltpu.make_async_copy(blocks.at[0, 0, slot], row, sems.at[0])
    side = pltpu.make_async_copy(rhs.at[0, 0, slot], head.at[:, 0:RHS], sems.at[1])
    whole.start()
    side.start()
    whole.wait()
    side.wait()
    head[:, RHS:] = row[:, 0 : HEAD * TILE]
    middle[...] = row[:, HEAD * TILE : LAST]
    last[...] = row[:, LAST:]


def pick(departure, blocks, rhs):
    return pl.pallas_call(
        pick_kernel,
        in_specs=[SMEM_SPEC] + [ANY_SPEC] * 2,
        out_specs=[VMEM_SPEC] * 3,
        out_shape=[
            vmem((DOF, RHS + HEAD * TILE), jnp.bfloat16),
            vmem((DOF, LAST - HEAD * TILE), jnp.bfloat16),
            vmem((DOF, DOF), jnp.bfloat16),
        ],
        scratch_shapes=[pltpu.VMEM((DOF, WIDE), jnp.bfloat16), pltpu.SemaphoreType.DMA((2,))],
        compiler_params=PARAMS,
        name="pick",
    )(*far(departure, blocks, rhs))


def first_kernel(arrival, rhs, lower, upper, kept, rounded):
    for q in range(KEPT):
        source = arrival[0, 0, q]

        @pl.when(source < 3)
        def _():
            kept[q] = rhs[0, 0, jnp.clip(source, 0, 2)]

        @pl.when(source == 3)
        def _():
            kept[q] = lower[:, 0:RHS]

        @pl.when(source == 4)
        def _():
            kept[q] = upper[:, 0:RHS]

        rounded[q] = (RELAXATION * kept[q].astype(jnp.float32)).astype(jnp.bfloat16)


def first(arrival, rhs, lower, upper):
    pair = vmem((KEPT, DOF, RHS), jnp.bfloat16)
    return pl.pallas_call(
        first_kernel,
        in_specs=[SMEM_SPEC] + [VMEM_SPEC] * 3,
        out_specs=[VMEM_SPEC] * 2,
        out_shape=[pair, pair],
        compiler_params=PARAMS,
        name="first",
    )(arrival, *near(rhs, lower, upper))


def local_kernel(arrival, neighbors, orientation, blocks, merged, rows, acc, sems):
    copies = [
        pltpu.make_async_copy(blocks.at[0, 0, jnp.clip(arrival[0, 0, q], 0, 2)], rows.at[q], sems.at[q])
        for q in range(KEPT)
    ]
    for copy in copies:
        copy.start()
    for q in range(KEPT):
        copies[q].wait()

        @pl.when(arrival[0, 0, q] < 3)
        def _():
            columns = lambda low, high: rows[q, :, low:high]
            put_own(columns, acc)
            neighbor = lambda face: neighbors[0, 0, q, face]
            turn = lambda face: orientation[0, 0, q, face]
            add_faces(range(FACES), columns, neighbor, turn, acc)
            for tile in range(TILES):
                merged[q, :, tile * TILE : (tile + 1) * TILE] = acc[tile].astype(jnp.bfloat16)


def merged_local(arrival, neighbors, orientation, blocks):
    return pl.pallas_call(
        local_kernel,
        in_specs=[SMEM_SPEC] * 3 + [ANY_SPEC],
        out_specs=VMEM_SPEC,
        out_shape=vmem((KEPT, DOF, MERGED), jnp.bfloat16),
        scratch_shapes=[
            pltpu.VMEM((KEPT, DOF, WIDE), jnp.bfloat16),
            pltpu.VMEM((TILES, DOF, TILE), jnp.float32),
            pltpu.SemaphoreType.DMA((KEPT,)),
        ],
        compiler_params=PARAMS,
        name="merge_local",
    )(arrival, neighbors, orientation, *far(blocks))


def arrived_kernel(
    arrival, neighbors, orientation, local, lo_head, lo_middle, hi_head, hi_middle, merged, acc
):
    del local
    for q in range(KEPT):
        for code, head, middle in ((3, lo_head, lo_middle), (4, hi_head, hi_middle)):

            @pl.when(arrival[0, 0, q] == code)
            def _():
                def columns(low, high):
                    if high <= HEAD * TILE:
                        return head[:, RHS + low : RHS + high]
                    return middle[:, low - HEAD * TILE : high - HEAD * TILE]

                put_own(columns, acc.at[q])
                neighbor = lambda face: neighbors[0, 0, q, face]
                turn = lambda face: orientation[0, 0, q, face]
                add_faces(range(FACES - 1), columns, neighbor, turn, acc.at[q])
                for tile in range(TILES):
                    merged[q, :, tile * TILE : (tile + 1) * TILE] = acc[q, tile].astype(jnp.bfloat16)


def merged_arrived(arrival, neighbors, orientation, local, lo_head, lo_middle, hi_head, hi_middle):
    return pl.pallas_call(
        arrived_kernel,
        in_specs=[SMEM_SPEC] * 3 + [VMEM_SPEC] * 5,
        out_specs=[VMEM_SPEC] * 2,
        out_shape=[
            vmem((KEPT, DOF, MERGED), jnp.bfloat16),
            vmem((KEPT, TILES, DOF, TILE), jnp.float32),
        ],
        input_output_aliases={3: 0},
        compiler_params=PARAMS,
        name="merge_arrived",
    )(arrival, neighbors, orientation, *near(local, lo_head, lo_middle, hi_head, hi_middle))


def applied_rows(merged, own, below, above):
    far = jnp.concatenate([below[0], below[1], above[0], above[1]], axis=0)
    for q in range(KEPT):
        near = jnp.concatenate([own[q], own[1 - q]], axis=0)
        applied = jnp.dot(merged[q, :, 0 : 2 * DOF], near, preferred_element_type=jnp.float32)
        applied += jnp.dot(merged[q, :, 2 * DOF :], far, preferred_element_type=jnp.float32)
        yield q, applied


def opening_kernel(
    arrival, neighbors, orientation, partial, acc, lo_last, hi_last, kept, own, below, above, merged, iterate, rounded
):
    del partial
    for q in range(KEPT):
        for code, last in ((3, lo_last), (4, hi_last)):

            @pl.when(arrival[0, 0, q] == code)
            def _():
                face = FACES - 1
                tile, select = turned_select(LAST, neighbors[0, 0, q, face], orientation[0, 0, q, face])
                moved = jnp.dot(last[...], select, preferred_element_type=jnp.float32)
                for part in range(SPAN):
                    total = acc[q, tile + part] + moved[:, part * TILE : (part + 1) * TILE]
                    place = pl.multiple_of((tile + part) * TILE, TILE)
                    merged[q, :, pl.ds(place, TILE)] = total.astype(jnp.bfloat16)

    for q, applied in applied_rows(merged, own, below, above):
        side = kept[q].astype(jnp.float32)
        value = RELAXATION * side + RELAXATION * (side - applied)
        iterate[q] = value
        rounded[q] = value.astype(jnp.bfloat16)


def opening(arrival, neighbors, orientation, partial, acc, lo_last, hi_last, kept, own, below, above):
    return pl.pallas_call(
        opening_kernel,
        in_specs=[SMEM_SPEC] * 3 + [VMEM_SPEC] * 8,
        out_specs=[VMEM_SPEC] * 3,
        out_shape=[
            vmem((KEPT, DOF, MERGED), jnp.bfloat16),
            vmem((KEPT, DOF, RHS), jnp.float32),
            vmem((KEPT, DOF, RHS), jnp.bfloat16),
        ],
        input_output_aliases={3: 0},
        compiler_params=PARAMS,
        name="opening",
    )(arrival, neighbors, orientation, *near(partial, acc, lo_last, hi_last, kept, own, below, above))


def middle_kernel(merged, kept, iterate, own, below, above, iterate_out, rounded):
    for q, applied in applied_rows(merged, own, below, above):
        value = iterate[q] + RELAXATION * (kept[q].astype(jnp.float32) - applied)
        iterate_out[q] = value
        rounded[q] = value.astype(jnp.bfloat16)


def middle(merged, kept, iterate, own, below, above):
    return pl.pallas_call(
        middle_kernel,
        in_specs=[VMEM_SPEC] * 6,
        out_specs=[VMEM_SPEC] * 2,
        out_shape=[vmem((KEPT, DOF, RHS), jnp.float32), vmem((KEPT, DOF, RHS), jnp.bfloat16)],
        compiler_params=PARAMS,
        name="middle",
    )(*near(merged, kept, iterate, own, below, above))


def closing_kernel(merged, kept, iterate, own, below, above, smoothed):
    for q, applied in applied_rows(merged, own, below, above):
        smoothed[0, 0, q] = iterate[q] + RELAXATION * (kept[q].astype(jnp.float32) - applied)


def closing(merged, kept, iterate, own, below, above):
    return pl.pallas_call(
        closing_kernel,
        in_specs=[VMEM_SPEC] * 6,
        out_specs=VMEM_SPEC,
        out_shape=jax.ShapeDtypeStruct((1, 1, KEPT, DOF, RHS), jnp.float32),
        compiler_params=PARAMS,
        name="closing",
    )(*near(merged, kept, iterate, own, below, above))


def shifted(value, axis, steps, closed):
    count = lax.axis_size(axis)
    pairs = [(source, (source + steps) % count) for source in range(count)]
    if not closed:
        pairs = [(source, target) for source, target in pairs if target == source + steps]
    return lax.ppermute(value, axis, pairs)


def halo(rounded):
    below = shifted(rounded, "gx", 1, closed=True)
    above = shifted(rounded, "gx", -1, closed=True)
    return below, above


def both_ways(value):
    lower = shifted(value, "gy", 1, closed=False)
    upper = shifted(value, "gy", -1, closed=False)
    return lower, upper


def shards(blocks, right_side, departure, arrival, neighbors, orientation):
    head, middle_columns, last = pick(departure, blocks, right_side)
    lo_head, hi_head = both_ways(head)
    lo_middle, hi_middle = both_ways(middle_columns)
    lo_last, hi_last = both_ways(last)
    kept, own = first(arrival, right_side, lo_head, hi_head)
    below, above = halo(own)
    local = merged_local(arrival, neighbors, orientation, blocks)
    partial, acc = merged_arrived(
        arrival, neighbors, orientation, local, lo_head, lo_middle, hi_head, hi_middle
    )
    merged, iterate, own = opening(
        arrival, neighbors, orientation, partial, acc, lo_last, hi_last, kept, own, below, above
    )
    for _ in range(1, ITERS - 1):
        below, above = halo(own)
        iterate, own = middle(merged, kept, iterate, own, below, above)
    below, above = halo(own)
    return closing(merged, kept, iterate, own, below, above)


def solution(mesh):
    in_specs = (
        P("gx", "gy", None, None, None),
        P("gx", "gy", None, None, None),
        P("gx", "gy", None),
        P("gx", "gy", None),
        P("gx", "gy", None, None),
        P("gx", "gy", None, None),
    )
    out_specs = P("gx", "gy", None, None, None)
    return jax.shard_map(shards, mesh=mesh, in_specs=in_specs, out_specs=out_specs, check_vma=False)
```

```python
import jax
import jax.numpy as jnp
from jax import lax
from jax.experimental import pallas as pl
from jax.experimental.pallas import tpu as pltpu
from jax.sharding import PartitionSpec as P


DOF = 320
FACES = 6
RHS = 128
KEPT = 2
ITERS = 4
RELAXATION = 0.7
WIDE = 7 * DOF
TILE = 128
SLOTS = 6
MERGED = SLOTS * DOF
TILES = MERGED // TILE
OWN = DOF // TILE
HEAD = 5
SPAN = 3
LAST = DOF * FACES


def vmem(shape, dtype):
    return pltpu.VMEM(shape, dtype)


def near(*arrays):
    return tuple(pltpu.with_memory_space_constraint(array, pltpu.VMEM) for array in arrays)


def far(*arrays):
    return tuple(pltpu.with_memory_space_constraint(array, pltpu.HBM) for array in arrays)


PARAMS = pltpu.CompilerParams(vmem_limit_bytes=20 * 2**20)

SMEM_SPEC = pl.BlockSpec(memory_space=pltpu.SMEM)
VMEM_SPEC = pl.BlockSpec(memory_space=pltpu.VMEM)
ANY_SPEC = pl.BlockSpec(memory_space=pl.ANY)


def turned_select(start, n, k):
    shift = start % TILE
    layer = n // 2
    here = lax.axis_index("gx")
    outside = ((layer == 0) & (here == 0)) | ((layer == 2) & (here == lax.axis_size("gx") - 1))
    slot = jnp.where(layer == 1, 1, jnp.where(layer == 0, 2, 4) + n % 2)
    place = DOF * slot
    tile = place // TILE
    column = lax.broadcasted_iota(jnp.int32, (1, SPAN * TILE), 1) - (place - tile * TILE)
    a = (column // 16) % 4
    b = (column // 4) % 4
    source_a = jnp.where(k == 0, a, jnp.where(k == 1, 3 - b, jnp.where(k == 2, 3 - a, b)))
    source_b = jnp.where(k == 0, b, jnp.where(k == 1, a, jnp.where(k == 2, 3 - b, 3 - a)))
    source = shift + (column // 64) * 64 + source_a * 16 + source_b * 4 + column % 4
    source = jnp.where((column >= 0) & (column < DOF) & jnp.logical_not(outside), source, -1)
    rows = lax.broadcasted_iota(jnp.int32, (DOF + shift, SPAN * TILE), 0)
    return tile, jnp.where(rows == source, 1.0, 0.0).astype(jnp.bfloat16)


def add_faces(faces, columns, neighbor, turn, acc_ref):
    for face in faces:
        start = DOF * (face + 1)
        tile, select = turned_select(start, neighbor(face), turn(face))
        base = start - start % TILE
        moved = jnp.dot(columns(base, start + DOF), select, preferred_element_type=jnp.float32)
        for part in range(SPAN):
            acc_ref[tile + part] += moved[:, part * TILE : (part + 1) * TILE]


def put_own(columns, acc_ref):
    lane = lax.broadcasted_iota(jnp.int32, (DOF, TILE), 1)
    for tile in range(TILES):
        if tile <= OWN:
            acc_ref[tile] = columns(tile * TILE, (tile + 1) * TILE).astype(jnp.float32)
        else:
            acc_ref[tile] = jnp.zeros((DOF, TILE), jnp.float32)
    acc_ref[OWN] = jnp.where(lane < DOF - OWN * TILE, acc_ref[OWN], 0.0)


def pick_kernel(departure, blocks, rhs, head, middle, last, row, sems):
    slot = jnp.maximum(jnp.maximum(departure[0, 0, 0], departure[0, 0, 1]), 0)
    whole = pltpu.make_async_copy(blocks.at[0, 0, slot], row, sems.at[0])
    side = pltpu.make_async_copy(rhs.at[0, 0, slot], head.at[:, 0:RHS], sems.at[1])
    whole.start()
    side.start()
    whole.wait()
    side.wait()
    head[:, RHS:] = row[:, 0 : HEAD * TILE]
    middle[...] = row[:, HEAD * TILE : LAST]
    for part in range(OWN):
        last[part * DOF : (part + 1) * DOF] = row[:, LAST + part * TILE : LAST + (part + 1) * TILE]
    rest = row[:, LAST + OWN * TILE :]
    last[OWN * DOF :] = jnp.concatenate([rest[: DOF // 2], rest[DOF // 2 :]], axis=1)


def pick(departure, blocks, rhs):
    return pl.pallas_call(
        pick_kernel,
        in_specs=[SMEM_SPEC] + [ANY_SPEC] * 2,
        out_specs=[VMEM_SPEC] * 3,
        out_shape=[
            vmem((DOF, RHS + HEAD * TILE), jnp.bfloat16),
            vmem((DOF, LAST - HEAD * TILE), jnp.bfloat16),
            vmem((DOF * DOF // TILE, TILE), jnp.bfloat16),
        ],
        scratch_shapes=[pltpu.VMEM((DOF, WIDE), jnp.bfloat16), pltpu.SemaphoreType.DMA((2,))],
        compiler_params=PARAMS,
        name="pick",
    )(*far(departure, blocks, rhs))


def first_kernel(arrival, rhs, lower, upper, kept, rounded):
    for q in range(KEPT):
        source = arrival[0, 0, q]

        @pl.when(source < 3)
        def _():
            kept[q] = rhs[0, 0, jnp.clip(source, 0, 2)]

        @pl.when(source == 3)
        def _():
            kept[q] = lower[:, 0:RHS]

        @pl.when(source == 4)
        def _():
            kept[q] = upper[:, 0:RHS]

        rounded[q] = (RELAXATION * kept[q].astype(jnp.float32)).astype(jnp.bfloat16)


def first(arrival, rhs, lower, upper):
    pair = vmem((KEPT, DOF, RHS), jnp.bfloat16)
    return pl.pallas_call(
        first_kernel,
        in_specs=[SMEM_SPEC] + [VMEM_SPEC] * 3,
        out_specs=[VMEM_SPEC] * 2,
        out_shape=[pair, pair],
        compiler_params=PARAMS,
        name="first",
    )(arrival, *near(rhs, lower, upper))


def local_kernel(arrival, neighbors, orientation, blocks, merged, rows, acc, sems):
    copies = [
        pltpu.make_async_copy(blocks.at[0, 0, jnp.clip(arrival[0, 0, q], 0, 2)], rows.at[q], sems.at[q])
        for q in range(KEPT)
    ]
    for copy in copies:
        copy.start()
    for q in range(KEPT):
        copies[q].wait()

        @pl.when(arrival[0, 0, q] < 3)
        def _():
            columns = lambda low, high: rows[q, :, low:high]
            put_own(columns, acc)
            neighbor = lambda face: neighbors[0, 0, q, face]
            turn = lambda face: orientation[0, 0, q, face]
            add_faces(range(FACES), columns, neighbor, turn, acc)
            for tile in range(TILES):
                merged[q, :, tile * TILE : (tile + 1) * TILE] = acc[tile].astype(jnp.bfloat16)


def merged_local(arrival, neighbors, orientation, blocks):
    return pl.pallas_call(
        local_kernel,
        in_specs=[SMEM_SPEC] * 3 + [ANY_SPEC],
        out_specs=VMEM_SPEC,
        out_shape=vmem((KEPT, DOF, MERGED), jnp.bfloat16),
        scratch_shapes=[
            pltpu.VMEM((KEPT, DOF, WIDE), jnp.bfloat16),
            pltpu.VMEM((TILES, DOF, TILE), jnp.float32),
            pltpu.SemaphoreType.DMA((KEPT,)),
        ],
        compiler_params=PARAMS,
        name="merge_local",
    )(arrival, neighbors, orientation, *far(blocks))


def arrived_kernel(
    arrival, neighbors, orientation, local, lo_head, lo_middle, hi_head, hi_middle, merged, acc
):
    del local
    for q in range(KEPT):
        for code, head, middle in ((3, lo_head, lo_middle), (4, hi_head, hi_middle)):

            @pl.when(arrival[0, 0, q] == code)
            def _():
                def columns(low, high):
                    if high <= HEAD * TILE:
                        return head[:, RHS + low : RHS + high]
                    return middle[:, low - HEAD * TILE : high - HEAD * TILE]

                put_own(columns, acc.at[q])
                neighbor = lambda face: neighbors[0, 0, q, face]
                turn = lambda face: orientation[0, 0, q, face]
                add_faces(range(FACES - 1), columns, neighbor, turn, acc.at[q])
                for tile in range(TILES):
                    merged[q, :, tile * TILE : (tile + 1) * TILE] = acc[q, tile].astype(jnp.bfloat16)


def merged_arrived(arrival, neighbors, orientation, local, lo_head, lo_middle, hi_head, hi_middle):
    return pl.pallas_call(
        arrived_kernel,
        in_specs=[SMEM_SPEC] * 3 + [VMEM_SPEC] * 5,
        out_specs=[VMEM_SPEC] * 2,
        out_shape=[
            vmem((KEPT, DOF, MERGED), jnp.bfloat16),
            vmem((KEPT, TILES, DOF, TILE), jnp.float32),
        ],
        input_output_aliases={3: 0},
        compiler_params=PARAMS,
        name="merge_arrived",
    )(arrival, neighbors, orientation, *near(local, lo_head, lo_middle, hi_head, hi_middle))


def applied_rows(merged, own, below, above):
    far = jnp.concatenate([below[0], below[1], above[0], above[1]], axis=0)
    for q in range(KEPT):
        near = jnp.concatenate([own[q], own[1 - q]], axis=0)
        applied = jnp.dot(merged[q, :, 0 : 2 * DOF], near, preferred_element_type=jnp.float32)
        applied += jnp.dot(merged[q, :, 2 * DOF :], far, preferred_element_type=jnp.float32)
        yield q, applied


def last_moved(last, select):
    whole = jnp.concatenate([last[part * DOF : (part + 1) * DOF] for part in range(OWN)], axis=1)
    moved = jnp.dot(whole, select[: OWN * TILE], preferred_element_type=jnp.float32)
    rest = last[OWN * DOF :]
    edge = select[OWN * TILE :]
    empty = jnp.zeros_like(edge)
    upper = jnp.dot(rest, jnp.concatenate([edge, empty], axis=0), preferred_element_type=jnp.float32)
    lower = jnp.dot(rest, jnp.concatenate([empty, edge], axis=0), preferred_element_type=jnp.float32)
    return moved + jnp.concatenate([upper, lower], axis=0)


def opening_kernel(
    arrival, neighbors, orientation, partial, acc, lo_last, hi_last, kept, own, below, above, merged, iterate, rounded
):
    del partial
    for q in range(KEPT):
        for code, last in ((3, lo_last), (4, hi_last)):

            @pl.when(arrival[0, 0, q] == code)
            def _():
                face = FACES - 1
                tile, select = turned_select(LAST, neighbors[0, 0, q, face], orientation[0, 0, q, face])
                moved = last_moved(last, select)
                for part in range(SPAN):
                    total = acc[q, tile + part] + moved[:, part * TILE : (part + 1) * TILE]
                    place = pl.multiple_of((tile + part) * TILE, TILE)
                    merged[q, :, pl.ds(place, TILE)] = total.astype(jnp.bfloat16)

    for q, applied in applied_rows(merged, own, below, above):
        side = kept[q].astype(jnp.float32)
        value = RELAXATION * side + RELAXATION * (side - applied)
        iterate[q] = value
        rounded[q] = value.astype(jnp.bfloat16)


def opening(arrival, neighbors, orientation, partial, acc, lo_last, hi_last, kept, own, below, above):
    return pl.pallas_call(
        opening_kernel,
        in_specs=[SMEM_SPEC] * 3 + [VMEM_SPEC] * 8,
        out_specs=[VMEM_SPEC] * 3,
        out_shape=[
            vmem((KEPT, DOF, MERGED), jnp.bfloat16),
            vmem((KEPT, DOF, RHS), jnp.float32),
            vmem((KEPT, DOF, RHS), jnp.bfloat16),
        ],
        input_output_aliases={3: 0},
        compiler_params=PARAMS,
        name="opening",
    )(arrival, neighbors, orientation, *near(partial, acc, lo_last, hi_last, kept, own, below, above))


def middle_kernel(merged, kept, iterate, own, below, above, iterate_out, rounded):
    for q, applied in applied_rows(merged, own, below, above):
        value = iterate[q] + RELAXATION * (kept[q].astype(jnp.float32) - applied)
        iterate_out[q] = value
        rounded[q] = value.astype(jnp.bfloat16)


def middle(merged, kept, iterate, own, below, above):
    return pl.pallas_call(
        middle_kernel,
        in_specs=[VMEM_SPEC] * 6,
        out_specs=[VMEM_SPEC] * 2,
        out_shape=[vmem((KEPT, DOF, RHS), jnp.float32), vmem((KEPT, DOF, RHS), jnp.bfloat16)],
        compiler_params=PARAMS,
        name="middle",
    )(*near(merged, kept, iterate, own, below, above))


def closing_kernel(merged, kept, iterate, own, below, above, smoothed, values, sems):
    copies = [pltpu.make_async_copy(values.at[q], smoothed.at[0, 0, q], sems.at[q]) for q in range(KEPT)]
    for q, applied in applied_rows(merged, own, below, above):
        values[q] = iterate[q] + RELAXATION * (kept[q].astype(jnp.float32) - applied)
        copies[q].start()
    for copy in copies:
        copy.wait()


def closing(merged, kept, iterate, own, below, above):
    return pl.pallas_call(
        closing_kernel,
        in_specs=[VMEM_SPEC] * 6,
        out_specs=ANY_SPEC,
        out_shape=jax.ShapeDtypeStruct((1, 1, KEPT, DOF, RHS), jnp.float32),
        scratch_shapes=[pltpu.VMEM((KEPT, DOF, RHS), jnp.float32), pltpu.SemaphoreType.DMA((KEPT,))],
        compiler_params=PARAMS,
        name="closing",
    )(*near(merged, kept, iterate, own, below, above))


def shifted(value, axis, steps, closed):
    count = lax.axis_size(axis)
    pairs = [(source, (source + steps) % count) for source in range(count)]
    if not closed:
        pairs = [(source, target) for source, target in pairs if target == source + steps]
    return lax.ppermute(value, axis, pairs)


def halo(rounded):
    below = shifted(rounded, "gx", 1, closed=True)
    above = shifted(rounded, "gx", -1, closed=True)
    return below, above


def both_ways(value):
    lower = shifted(value, "gy", 1, closed=False)
    upper = shifted(value, "gy", -1, closed=False)
    return lower, upper


def shards(blocks, right_side, departure, arrival, neighbors, orientation):
    head, middle_columns, last = pick(departure, blocks, right_side)
    lo_head, hi_head = both_ways(head)
    lo_middle, hi_middle = both_ways(middle_columns)
    lo_last, hi_last = both_ways(last)
    kept, own = first(arrival, right_side, lo_head, hi_head)
    below, above = halo(own)
    local = merged_local(arrival, neighbors, orientation, blocks)
    partial, acc = merged_arrived(
        arrival, neighbors, orientation, local, lo_head, lo_middle, hi_head, hi_middle
    )
    merged, iterate, own = opening(
        arrival, neighbors, orientation, partial, acc, lo_last, hi_last, kept, own, below, above
    )
    for _ in range(1, ITERS - 1):
        below, above = halo(own)
        iterate, own = middle(merged, kept, iterate, own, below, above)
    below, above = halo(own)
    return closing(merged, kept, iterate, own, below, above)


def solution(mesh):
    in_specs = (
        P("gx", "gy", None, None, None),
        P("gx", "gy", None, None, None),
        P("gx", "gy", None),
        P("gx", "gy", None),
        P("gx", "gy", None, None),
        P("gx", "gy", None, None),
    )
    out_specs = P("gx", "gy", None, None, None)
    return jax.shard_map(shards, mesh=mesh, in_specs=in_specs, out_specs=out_specs, check_vma=False)
```
